32 devices in a mesh: lat: 4 (over z), lon: 8 (over y, x, core).
Axes of the slice: x: 2, y: 2, z: 4, core: 2. Of those that a mesh axis runs over, the one named last changes fastest.
Arguments:
- observations: bfloat16 [49152, 128], P(('lat', 'lon')), may hold values from -6 to 6
- owner_device: int32 [49152, 1], P(('lat', 'lon')), may hold values from 0 to 31; in each aligned block of 1536 rows (0 to 1535, 1536 to 3071, ...) at most 96 rows name the same one
- local_cell: int32 [49152], P(('lat', 'lon')), may hold values from 0 to 383
- valid_counts: int32 [32], P(('lat', 'lon')), may hold values from 768 to 1536
- weight_in: bfloat16 [128, 256], replicated, may hold values from -0.5 to 0.5
- bias_in: float32 [256], replicated, may hold values from -3 to 3
- weight_out: bfloat16 [256, 256], replicated, may hold values from -0.375 to 0.375
- kernel_taps: float32 [9, 256], replicated, may hold values from -2 to 2
- cotangent: bfloat16 [64, 192, 256], P(('lat', 'lon')), may hold values from -6 to 6
Outputs:
- grid_out: bfloat16 [64, 192, 256], P(('lat', 'lon'))
- grad_weight_in: float32 [128, 256], replicated
- grad_bias_in: float32 [256], replicated
- grad_weight_out: float32 [256, 256], replicated
- grad_kernel: float32 [9, 256], replicated
The draws below stay inside these ranges and needn't reach their ends.
Inputs may be any that keep to these rules, and one draw needn't show every extreme that they name: `owner_device`: within the rows of one block, at most 96 rows name one owner, and in every draw some block names some owner exactly 96 times.
All inputs are finite; a program needn't handle non-finite values.
Results may differ from the reference program's by a relative error of at most 0.0065.
Values may be sent and summed in bfloat16 or wider, within the bound.
A program may use at most 64 MiB of HBM per device.

```python
import math
import jax
import jax.numpy as jnp
import numpy as np
from jax import lax

FEAT = 128
HIDDEN_SIZE = 256
CHANNELS = 256
TAPS = 9
TLAT = 16
TLON = 24
OBS_DEV = 1536
GLAT = 64
GLON = 192
OBS_ALL = 49152
CAP = 96
N_LAT = 4
N_LON = 8


def with_ends(result, rng, low, high):
    extent = result.shape
    spot = [jax.random.randint(jax.random.fold_in(rng, axis), (), 0, extent[axis]) for axis in range(len(extent))]
    result = result.at[tuple(spot)].set(low)
    longest = extent.index(max(extent))
    spot[longest] = (spot[longest] + 1) % extent[longest]
    return result.at[tuple(spot)].set(high)


def levels(rng, shape, shards, least, top_value):
    factor_of, own = 1.0, jax.random.fold_in(rng, 6)
    for axis_at, parts in shards:
        heights = jnp.exp(jax.random.uniform(jax.random.fold_in(own, axis_at), (parts,), jnp.float32, least / len(shards), top_value / len(shards)))
        factor_of = factor_of * jnp.repeat(heights, shape[axis_at] // parts).reshape([-1 if axis == axis_at else 1 for axis in range(len(shape))])
    return factor_of


def deal_out(stream_key, own, number, rows, count, top, reach, slope):
    sequence = jax.random.permutation(stream_key, count)
    packed, ordinary = portions_of(count, rows * top, reach, slope, True), portions_of(count, rows * top, reach, slope, False)
    places = jnp.arange(count)

    def named(sizes, turn):
        used = int((sizes > 0).sum())
        fixed = max(1, used // 4)
        shifted = fixed + (places - fixed + turn * (used - fixed)) % max(1, count - fixed)
        return jnp.zeros((count,), jnp.int32).at[sequence[jnp.where(places < fixed, places, shifted)]].set(jnp.asarray(sizes, jnp.int32))

    sizes = jnp.where(number % 4 == 0, named(packed, number // 4), named(ordinary, number - number // 4 - 1))
    mixed = jax.random.permutation(jax.random.fold_in(own, 3), count)
    source_of, taker = mixed[0:count // 2 * 2:2], mixed[1:count // 2 * 2:2]
    room = jnp.minimum(sizes[source_of] - 1, reach - sizes[taker]) // 2
    room = jnp.where((source_of == sequence[0]) | (taker == sequence[0]) | (sizes[taker] == 0), 0, jnp.maximum(room, 0))
    shifted = jax.random.randint(jax.random.fold_in(own, 4), (count // 2,), 0, 1 << 20) % (room + 1)
    sizes = sizes.at[source_of].add(-shifted).at[taker].add(shifted)
    items = jnp.searchsorted(jnp.cumsum(sizes), jnp.arange(rows * top), side="right").astype(jnp.int32)
    grid = items.reshape(top, rows).T
    grid = grid[jax.random.permutation(jax.random.fold_in(own, 1), rows)]
    turn = jax.random.randint(jax.random.fold_in(own, 2), (rows, 1), 0, top)
    return jnp.take_along_axis(grid, (jnp.arange(top)[None, :] + turn) % top, axis=1)


def portions_of(amount, total, limit, lean, full):
    weights = [(1 << 20) // math.isqrt(standing ** lean) + 1 for standing in range(1, amount + 1)]
    largest = limit if full else min(limit, max(-(-total // amount), total * weights[0] // sum(weights)))
    least = 1 if total - largest >= amount - 1 else 0
    counts, surplus = [largest] + [least] * (amount - 1), total - largest - least * (amount - 1)
    while surplus > 0:
        movable = [i for i in range(1, amount) if counts[i] < largest] or [i for i in range(1, amount) if counts[i] < limit]
        whole, left = sum([weights[i] for i in movable]), surplus
        for i in movable:
            extra = min(limit - counts[i], max(1, left * weights[i] // whole), surplus)
            counts[i] = counts[i] + extra
            surplus = surplus - extra
    return np.array(counts)


def bell_draw(own_key, shape, width, bound, split=(), kind=jnp.bfloat16):
    array = width * jax.random.normal(own_key, shape, jnp.float32)
    if split:
        array = array * levels(own_key, shape, split, -0.22, 0.18)
    return jnp.clip(array, -bound, bound).astype(kind)


def setup_inputs(seed: int = 0) -> dict:
    splits = jax.random.split(jax.random.key(seed), 10)
    observations = bell_draw(splits[0], (OBS_ALL, FEAT), 1.0, 6.0, ((0, 32),))
    owner_device_keys = jax.random.split(jax.random.fold_in(splits[1], 1), OBS_ALL // OBS_DEV)
    owner_device_turns = jax.random.permutation(jax.random.fold_in(splits[1], 3), OBS_ALL // OBS_DEV)
    owner_device = jax.vmap(lambda own, number: deal_out(jax.random.fold_in(splits[1], 2), own, number, OBS_DEV, N_LAT * N_LON, 1, CAP, 2))(owner_device_keys, owner_device_turns).reshape((OBS_ALL, 1))
    local_cell = with_ends(jax.random.randint(splits[2], (OBS_ALL,), 0, TLAT * TLON), jax.random.fold_in(splits[2], 1), 0, (TLAT * TLON) - 1).astype(jnp.int32)
    valid_counts = with_ends(jax.random.randint(splits[3], (N_LAT * N_LON,), OBS_DEV // 2, OBS_DEV + 1), jax.random.fold_in(splits[3], 1), OBS_DEV // 2, OBS_DEV).astype(jnp.int32)
    weight_in = bell_draw(splits[4], (FEAT, HIDDEN_SIZE), FEAT ** -0.5, 0.5)
    bias_in = bell_draw(splits[5], (HIDDEN_SIZE,), 0.5, 3.0, (), jnp.float32)
    weight_out = bell_draw(splits[6], (HIDDEN_SIZE, CHANNELS), HIDDEN_SIZE ** -0.5, 0.375)
    kernel_taps = bell_draw(splits[7], (TAPS, CHANNELS), 0.33, 2.0, (), jnp.float32)
    cotangent = bell_draw(splits[8], (GLAT, GLON, CHANNELS), 1.0, 6.0, ((0, 32),))
    return {"observations": observations, "owner_device": owner_device, "local_cell": local_cell, "valid_counts": valid_counts, "weight_in": weight_in, "bias_in": bias_in, "weight_out": weight_out, "kernel_taps": kernel_taps, "cotangent": cotangent}


OFFSETS = [(shift_lat, shift_lon) for shift_lat in (-1, 0, 1) for shift_lon in (-1, 0, 1)]

def pad_grid(values):
    wrapped = jnp.concatenate([values[:, -1:], values, values[:, :1]], axis=1)
    return jnp.pad(wrapped, ((1, 1), (0, 0), (0, 0)))

def encoder(rows, weight_in, bias_in, weight_out):
    before = jnp.dot(rows, weight_in, preferred_element_type=jnp.float32) + bias_in
    hidden = jax.nn.gelu(before).astype(jnp.bfloat16)
    encoded = jnp.dot(hidden, weight_out, preferred_element_type=jnp.float32).astype(jnp.bfloat16)
    return (before, hidden, encoded)

def local_grads(rows, before, hidden, upstream, weight_out):
    contract = (((0,), (0,)), ((), ()))
    grad_out = lax.dot_general(hidden, upstream, contract, preferred_element_type=jnp.float32)
    back = lax.dot_general(upstream, weight_out, (((1,), (1,)), ((), ())), preferred_element_type=jnp.float32)
    _, pullback = jax.vjp(jax.nn.gelu, before)
    pre_grad = pullback(back)[0].astype(jnp.bfloat16)
    grad_in = lax.dot_general(rows, pre_grad, contract, preferred_element_type=jnp.float32)
    grad_bias = lax.optimization_barrier(jnp.sum(pre_grad.astype(jnp.float32), axis=0))
    return (grad_in, grad_bias, grad_out)

def reference(observations, owner_device, local_cell, valid_counts, weight_in, bias_in, weight_out, kernel_taps, cotangent):
    devices_all = N_LAT * N_LON
    cells_total = GLAT * GLON
    row_blocks = observations.reshape(devices_all, OBS_DEV, FEAT)
    owner_blocks = owner_device.reshape(devices_all, OBS_DEV)
    local_blocks = local_cell.reshape(devices_all, OBS_DEV)

    def destination(owner_row, local_row, count):
        valid_rows = jnp.arange(OBS_DEV, dtype=jnp.int32) < count
        lat_cell = owner_row // N_LON * TLAT + local_row // TLON
        lon_cell = owner_row % N_LON * TLON + local_row % TLON
        return jnp.where(valid_rows, lat_cell * GLON + lon_cell, cells_total).astype(jnp.int32)

    def forward_step(deposit, item):
        rows, owner_row, local_row, count = item
        target = destination(owner_row, local_row, count)
        _, _, encoded = encoder(rows, weight_in, bias_in, weight_out)
        deposit = deposit + jax.ops.segment_sum(encoded.astype(jnp.float32), target, num_segments=cells_total + 1)
        return (deposit, None)
    deposit, _ = lax.scan(forward_step, jnp.zeros((cells_total + 1, CHANNELS), jnp.float32), (row_blocks, owner_blocks, local_blocks, valid_counts))
    point = deposit[:cells_total].reshape(GLAT, GLON, CHANNELS)
    padded = pad_grid(point)
    grid_field = jnp.zeros((GLAT, GLON, CHANNELS), jnp.float32)
    for tap_index, (shift_lat, shift_lon) in enumerate(OFFSETS):
        window = padded[1 + shift_lat:1 + shift_lat + GLAT, 1 + shift_lon:1 + shift_lon + GLON]
        grid_field = grid_field + kernel_taps[tap_index] * window
    grid_out = grid_field.astype(jnp.bfloat16)
    loss_scale = 1.0 / math.sqrt(OBS_DEV * devices_all)
    cot_float = cotangent.astype(jnp.float32)
    cot_padded = pad_grid(cot_float)
    kernel_rows = []
    adjoint = jnp.zeros((GLAT, GLON, CHANNELS), jnp.float32)
    for tap_index, (shift_lat, shift_lon) in enumerate(OFFSETS):
        window = padded[1 + shift_lat:1 + shift_lat + GLAT, 1 + shift_lon:1 + shift_lon + GLON]
        kernel_rows.append(loss_scale * lax.optimization_barrier(jnp.sum(cot_float * window, axis=(0, 1))))
        back_window = cot_padded[1 - shift_lat:1 - shift_lat + GLAT, 1 - shift_lon:1 - shift_lon + GLON]
        adjoint = adjoint + kernel_taps[tap_index] * back_window
    grad_kernel = jnp.stack(kernel_rows)
    adjoint = (loss_scale * adjoint).astype(jnp.bfloat16)
    adjoint_rows = jnp.concatenate([adjoint.reshape(cells_total, CHANNELS), jnp.zeros((1, CHANNELS), jnp.bfloat16)], axis=0)

    def backward_step(totals, item):
        rows, owner_row, local_row, count = item
        target = destination(owner_row, local_row, count)
        before, hidden, _ = encoder(rows, weight_in, bias_in, weight_out)
        upstream = adjoint_rows[target]
        grads = local_grads(rows, before, hidden, upstream, weight_out)
        return (tuple((total + grad for total, grad in zip(totals, grads))), None)
    zeros_start = (jnp.zeros((FEAT, HIDDEN_SIZE), jnp.float32), jnp.zeros((HIDDEN_SIZE,), jnp.float32), jnp.zeros((HIDDEN_SIZE, CHANNELS), jnp.float32))
    totals, _ = lax.scan(backward_step, zeros_start, (row_blocks, owner_blocks, local_blocks, valid_counts))
    return (grid_out, totals[0], totals[1], totals[2], grad_kernel)
```

```python
import functools
import math

import jax
import jax.numpy as jnp
from jax import lax
from jax.experimental import pallas as pl
from jax.experimental.pallas import tpu as pltpu
from jax.sharding import PartitionSpec as P

MESH = pl.DeviceIdType.MESH
F32 = jnp.float32
BF16 = jnp.bfloat16
OFFSETS = [(a, b) for a in (-1, 0, 1) for b in (-1, 0, 1)]
CURVE = math.sqrt(2.0 / math.pi)
META = 16
GROUP = 4


def round_up(value, step):
    return -(-value // step) * step


def iota(shape, dim):
    return lax.broadcasted_iota(jnp.int32, shape, dim)


def dot(left, right, contract=((1,), (0,))):
    return lax.dot_general(left, right, (contract, ((), ())), preferred_element_type=F32)


def kernel(
    n_lat, n_lon, slots, piece, scale,
    obs, owner, cell, count, w_in, b_in, w_out, taps, cot,
    grid_o, gin_o, gb_o, gout_o, gk_o,
    meta, slot_row, sbuf, rbuf, cot_top, cot_bot, adj_s, adj_r, adj_f, adj_b,
    dep, dep_b, dep_r, hal_top, hal_bot, strip, total, parts, gathered, gk_s, gk_r,
    row_send, row_recv, cot_send, cot_recv, adj_send, adj_recv, dep_send, dep_recv,
    hal_send, hal_recv, sum_send, sum_recv, all_send, all_recv, gk_send, gk_recv,
):
    n = n_lat * n_lon
    lat, lon = lax.axis_index("lat"), lax.axis_index("lon")
    me = lat * n_lon + lon
    obs_rows, feat = obs.shape
    own_rows, cols, channels = cot.shape
    tile_rows = own_rows * n_lon
    tile_cols = cols // n_lon
    cells = tile_rows * tile_cols
    hidden_size = w_in.shape[1]
    groups = n // GROUP

    def place(target):
        return (target // n_lon, lax.rem(target, n_lon))

    def remote(src, dst, send, recv, device):
        return pltpu.make_async_remote_copy(
            src_ref=src, dst_ref=dst, send_sem=send, recv_sem=recv,
            device_id=device, device_id_type=MESH,
        )

    def drain(ref, sem):
        pltpu.make_async_copy(ref, ref, sem).wait()

    barrier = pltpu.get_barrier_semaphore()

    def greet(off, carry):
        pl.semaphore_signal(
            barrier, inc=1, device_id=place(lax.rem(me + off, n)), device_id_type=MESH
        )
        return carry

    lax.fori_loop(1, n, greet, 0)

    @pl.when(me == 0)
    def _():
        cot_top[...] = jnp.zeros_like(cot_top)

    @pl.when(me == n - 1)
    def _():
        cot_bot[...] = jnp.zeros_like(cot_bot)

    has_top = jnp.logical_and(lon == 0, lat > 0)
    has_bot = jnp.logical_and(lon == n_lon - 1, lat < n_lat - 1)

    @pl.when(jnp.logical_not(has_top))
    def _():
        hal_top[...] = jnp.zeros_like(hal_top)

    @pl.when(jnp.logical_not(has_bot))
    def _():
        hal_bot[...] = jnp.zeros_like(hal_bot)

    dep[...] = jnp.zeros_like(dep)
    total[...] = jnp.zeros_like(total)
    dep_b[0] = jnp.zeros((tile_cols, channels), BF16)
    dep_b[tile_rows + 1] = jnp.zeros((tile_cols, channels), BF16)

    own_row = owner[...]
    match = (own_row == iota((n, obs_rows), 0)).astype(F32)
    block = 256 if obs_rows % 256 == 0 else 128
    upper = (iota((block, block), 0) < iota((block, block), 1)).astype(F32).astype(BF16)
    carry = jnp.zeros((n, 1), F32)
    ranks = []
    for start in range(0, obs_rows, block):
        part = match[:, start:start + block]
        before = dot(part.astype(BF16), upper) + carry
        ranks.append(jnp.sum(before * part, axis=0, keepdims=True))
        carry = carry + jnp.sum(part, axis=1, keepdims=True)
    rank = jnp.concatenate(ranks, axis=1).astype(jnp.int32)
    slot_row[...] = own_row * slots + rank
    lane = iota((1, obs_rows), 1)
    code = jnp.where(lane < count[0], cell[...] + 1, 0)
    high = (code // 128).astype(F32)
    low = lax.rem(code, 128).astype(F32)
    coded = jnp.concatenate([match * high, match * low], axis=0).astype(BF16)
    by_rank = (rank == iota((128, obs_rows), 0)).astype(F32).astype(BF16)
    meta[...] = dot(coded, by_rank, ((1,), (1,)))

    pl.semaphore_wait(barrier, n - 1)

    up_copy = remote(cot.at[own_rows - 1], cot_top, cot_send.at[0], cot_recv.at[0], place(lax.rem(me + 1, n)))
    down_copy = remote(cot.at[0], cot_bot, cot_send.at[1], cot_recv.at[1], place(lax.rem(me + n - 1, n)))

    @pl.when(me < n - 1)
    def _():
        up_copy.start()

    @pl.when(me > 0)
    def _():
        down_copy.start()

    def row_copy(off, g):
        return remote(
            sbuf.at[off], rbuf.at[off], row_send, row_recv.at[g], place(lax.rem(me + off, n))
        )

    def send_group(g, carry, first=False):
        ids = slot_row[...]
        picks = []
        for q in range(GROUP):
            target = lax.rem(me + g * GROUP + q, n)
            pick = (ids - target * slots) == iota((slots, obs_rows), 0)
            picks.append(pick.astype(F32).astype(BF16))
        rows = dot(jnp.concatenate(picks, axis=0), obs[...]).astype(BF16)
        line = iota((META, 128), 0)
        for q in range(GROUP):
            off = g * GROUP + q
            target = lax.rem(me + off, n)
            sbuf[off, :slots, :] = rows[q * slots:(q + 1) * slots]
            tail = jnp.where(
                line == 0, meta[pl.ds(target, 1), :],
                jnp.where(line == 1, meta[pl.ds(n + target, 1), :], 0.0),
            )
            sbuf[off, slots:slots + META, :] = tail.astype(BF16)
        for q in range(GROUP):
            if first and q == 0:
                pltpu.make_async_copy(sbuf.at[0], rbuf.at[0], row_recv.at[0]).start()
            else:
                row_copy(g * GROUP + q, g).start()
        return carry

    send_group(0, 0, True)

    @pl.when(me > 0)
    def _():
        up_copy.wait_recv()

    @pl.when(me < n - 1)
    def _():
        down_copy.wait_recv()

    tap = taps[...]

    def shifts(row):
        return {0: row, 1: pltpu.roll(row, 1, 0), -1: pltpu.roll(row, cols - 1, 0)}

    cot_rows = [cot_top[...]] + [cot[r] for r in range(own_rows)] + [cot_bot[...]]
    sums = [jnp.zeros((cols, channels), F32) for _ in range(own_rows)]
    for at, row in enumerate(cot_rows):
        moved = shifts(row.astype(F32))
        for y in range(own_rows):
            a = y - (at - 1)
            if abs(a) <= 1:
                for b in (-1, 0, 1):
                    k = 3 * (a + 1) + b + 1
                    sums[y] = sums[y] + tap[k:k + 1] * moved[b]
    for y in range(own_rows):
        value = scale * sums[y]
        for j in range(n_lon):
            adj_s[j, y] = value[j * tile_cols:(j + 1) * tile_cols].astype(BF16)

    def adj_copy(step):
        other = lax.rem(lon + step, n_lon)
        return remote(
            adj_s.at[other], adj_r.at[lon], adj_send, adj_recv, (lat, other)
        )

    for step in range(1, n_lon):
        adj_copy(step).start()
    adj_r[lon] = adj_s[lon]

    lax.fori_loop(1, groups, send_group, 0)

    drain(adj_r.at[pl.ds(0, n_lon - 1)], adj_recv)
    for k in range(n_lon):
        for y in range(own_rows):
            m = k * own_rows + y
            adj_f[m * tile_cols:(m + 1) * tile_cols, :] = adj_r[k, y].astype(F32)
    adj_b[...] = adj_f[...].astype(BF16)

    bias_at = hidden_size + feat

    def take_group(g, carry):
        held = rbuf.at[pl.ds(g * GROUP, GROUP)]
        drain(held, row_recv.at[g])
        rows = jnp.concatenate([rbuf[g * GROUP + q, :slots, :] for q in range(GROUP)], axis=0)
        same = iota((slots, 128), 0) == iota((slots, 128), 1)
        spread = []
        for q in range(GROUP):
            tail = rbuf[g * GROUP + q, slots:slots + META, :].astype(F32)
            spread.append(jnp.concatenate(
                [jnp.where(same, tail[0:1], 0.0), jnp.where(same, tail[1:2], 0.0)], axis=1
            ).astype(BF16))
        weigh = jnp.where(iota((256, 128), 0) < 128, 128.0, 1.0).astype(BF16)
        codes = dot(jnp.concatenate(spread, axis=0), weigh).astype(jnp.int32)
        lanes = iota(codes.shape, 1) + 1
        pick = jnp.concatenate(
            [(codes == lanes + at).astype(F32).astype(BF16) for at in range(0, cells, 128)], axis=1
        )
        x = dot(rows, w_in[...]) + b_in[...]
        square = x * x
        t = jnp.tanh(CURVE * (x + 0.044715 * (square * x)))
        half = 0.5 * (1.0 + t)
        hidden = (x * half).astype(BF16)
        slope = half + 0.5 * x * (1.0 - t * t) * (CURVE * (1.0 + 3.0 * 0.044715 * square))
        encoded = dot(hidden, w_out[...]).astype(BF16)
        dep[...] += dot(pick, encoded, ((0,), (0,)))
        upstream = dot(pick, adj_b[...]).astype(BF16)
        back = dot(upstream, w_out[...], ((1,), (1,)))
        pre = (back * slope).astype(BF16)
        total[0:hidden_size, :] += dot(hidden, upstream, ((0,), (0,)))
        total[hidden_size:bias_at, :] += dot(rows, pre, ((0,), (0,)))
        total[bias_at:bias_at + 1, :] += jnp.sum(pre.astype(F32), axis=0, keepdims=True)
        return carry

    lax.fori_loop(0, groups, take_group, 0)

    for m in range(tile_rows):
        dep_b[m + 1] = dep[m * tile_cols:(m + 1) * tile_cols, :].astype(BF16)

    def dep_copy(step):
        other = lax.rem(lon + step, n_lon)
        return remote(
            dep_b.at[pl.ds(other * own_rows, own_rows + 2)], dep_r.at[lon],
            dep_send, dep_recv, (lat, other),
        )

    low_copy = remote(
        dep_b.at[tile_rows], hal_top.at[lon], hal_send.at[0], hal_recv.at[0],
        (lax.rem(lat + 1, n_lat), 0),
    )
    high_copy = remote(
        dep_b.at[1], hal_bot.at[lon], hal_send.at[1], hal_recv.at[1],
        (lax.rem(lat + n_lat - 1, n_lat), n_lon - 1),
    )

    @pl.when(lat < n_lat - 1)
    def _():
        low_copy.start()

    @pl.when(lat > 0)
    def _():
        high_copy.start()

    for step in range(1, n_lon):
        dep_copy(step).start()
    dep_r[lon] = dep_b[pl.ds(lon * own_rows, own_rows + 2)]

    def span(at):
        return pl.ds(pl.multiple_of(at * piece, 8), piece)

    def sum_start(off, carry):
        target = lax.rem(me + off, n)
        remote(total.at[span(target)], parts.at[off - 1], sum_send, sum_recv, place(target)).start()
        return carry

    lax.fori_loop(1, n, sum_start, 0)

    drain(dep_r.at[pl.ds(0, n_lon - 1)], dep_recv)

    @pl.when(has_top)
    def _():
        drain(hal_top, hal_recv.at[0])

    @pl.when(has_bot)
    def _():
        drain(hal_bot, hal_recv.at[1])

    for j in range(n_lon):
        for r in range(own_rows + 2):
            value = dep_r[j, r].astype(F32)
            if r == 0:
                value = value + hal_top[j].astype(F32)
            if r == own_rows + 1:
                value = value + hal_bot[j].astype(F32)
            strip[r, j * tile_cols:(j + 1) * tile_cols, :] = value

    fields = [jnp.zeros((cols, channels), F32) for _ in range(own_rows)]
    kernel_rows = [jnp.zeros((1, channels), F32) for _ in OFFSETS]
    for at in range(own_rows + 2):
        moved = shifts(strip[at])
        for y in range(own_rows):
            a = at - 1 - y
            if abs(a) <= 1:
                for b in (-1, 0, 1):
                    k = 3 * (a + 1) + b + 1
                    fields[y] = fields[y] + tap[k:k + 1] * moved[-b]
                    kernel_rows[k] = kernel_rows[k] + jnp.sum(
                        cot[y].astype(F32) * moved[-b], axis=0, keepdims=True
                    )
    for y in range(own_rows):
        grid_o[y] = fields[y].astype(BF16)
    spare = gk_s.shape[0] - len(OFFSETS)
    gk_s[...] = scale * jnp.concatenate(kernel_rows + [jnp.zeros((spare, channels), F32)], axis=0)

    def gk_start(off, carry):
        target = lax.rem(me + off, n)
        remote(gk_s, gk_r.at[off - 1], gk_send, gk_recv, place(target)).start()
        return carry

    lax.fori_loop(1, n, gk_start, 0)

    drain(parts, sum_recv)

    def add_part(at, value):
        return value + parts[at]

    gathered[span(me), :] = lax.fori_loop(0, n - 1, add_part, total[span(me), :])

    def all_start(off, carry):
        target = lax.rem(me + off, n)
        remote(
            gathered.at[span(me)], gathered.at[span(me)], all_send, all_recv, place(target)
        ).start()
        return carry

    lax.fori_loop(1, n, all_start, 0)

    drain(gk_r, gk_recv)

    def add_kernel(at, value):
        return value + gk_r[at]

    gk_o[...] = lax.fori_loop(0, n - 1, add_kernel, gk_s[...])[0:len(OFFSETS)]

    drain(gathered.at[pl.ds(0, (n - 1) * piece)], all_recv)
    gout_o[...] = gathered[0:hidden_size, :]
    gin_o[...] = gathered[hidden_size:bias_at, :]
    gb_o[...] = gathered[bias_at:bias_at + 1, :]

    drain(sbuf.at[pl.ds(0, n - 1)], row_send)
    drain(adj_s.at[pl.ds(0, n_lon - 1)], adj_send)
    drain(dep_r.at[pl.ds(0, n_lon - 1)], dep_send)
    drain(parts, sum_send)
    drain(gathered.at[pl.ds(0, (n - 1) * piece)], all_send)
    drain(gk_r, gk_send)

    @pl.when(me < n - 1)
    def _():
        up_copy.wait_send()

    @pl.when(me > 0)
    def _():
        down_copy.wait_send()

    @pl.when(lat < n_lat - 1)
    def _():
        low_copy.wait_send()

    @pl.when(lat > 0)
    def _():
        high_copy.wait_send()


def local(
    observations, owner_device, local_cell, valid_counts,
    weight_in, bias_in, weight_out, kernel_taps, cotangent,
):
    n_lat, n_lon = lax.axis_size("lat"), lax.axis_size("lon")
    n = n_lat * n_lon
    obs_rows, feat = observations.shape
    hidden_size, channels = weight_out.shape
    own_rows, cols, _ = cotangent.shape
    tile_rows, tile_cols = own_rows * n_lon, cols // n_lon
    cells = tile_rows * tile_cols
    slots = round_up(2 * obs_rows // n, 16)
    piece = round_up(-(-(hidden_size + feat + 8) // n), 8)
    taps = kernel_taps.shape[0]
    kernel_pad = round_up(taps, 8)
    scale = 1.0 / math.sqrt(obs_rows * n)
    vmem = pl.BlockSpec(memory_space=pltpu.VMEM)
    dma = pltpu.SemaphoreType.DMA
    out = pl.pallas_call(
        functools.partial(kernel, n_lat, n_lon, slots, piece, scale),
        out_shape=(
            jax.ShapeDtypeStruct(cotangent.shape, BF16),
            jax.ShapeDtypeStruct((feat, hidden_size), F32),
            jax.ShapeDtypeStruct((1, hidden_size), F32),
            jax.ShapeDtypeStruct((hidden_size, channels), F32),
            jax.ShapeDtypeStruct((taps, channels), F32),
        ),
        in_specs=[vmem, vmem, vmem, pl.BlockSpec(memory_space=pltpu.SMEM)] + [vmem] * 5,
        out_specs=(vmem,) * 5,
        scratch_shapes=[
            pltpu.VMEM((2 * n, 128), F32),
            pltpu.VMEM((1, obs_rows), jnp.int32),
            pltpu.VMEM((n, slots + META, feat), BF16),
            pltpu.VMEM((n, slots + META, feat), BF16),
            pltpu.VMEM((cols, channels), BF16),
            pltpu.VMEM((cols, channels), BF16),
            pltpu.VMEM((n_lon, own_rows, tile_cols, channels), BF16),
            pltpu.VMEM((n_lon, own_rows, tile_cols, channels), BF16),
            pltpu.VMEM((cells, channels), F32),
            pltpu.VMEM((cells, channels), BF16),
            pltpu.VMEM((cells, channels), F32),
            pltpu.VMEM((tile_rows + 2, tile_cols, channels), BF16),
            pltpu.VMEM((n_lon, own_rows + 2, tile_cols, channels), BF16),
            pltpu.VMEM((n_lon, tile_cols, channels), BF16),
            pltpu.VMEM((n_lon, tile_cols, channels), BF16),
            pltpu.VMEM((own_rows + 2, cols, channels), F32),
            pltpu.VMEM((n * piece, channels), F32),
            pltpu.VMEM((n - 1, piece, channels), F32),
            pltpu.VMEM((n * piece, channels), F32),
            pltpu.VMEM((kernel_pad, channels), F32),
            pltpu.VMEM((n - 1, kernel_pad, channels), F32),
            dma, dma((n // GROUP,)), dma((2,)), dma((2,)), dma, dma, dma, dma,
            dma((2,)), dma((2,)), dma, dma, dma, dma, dma, dma,
        ],
        compiler_params=pltpu.CompilerParams(
            collective_id=0, has_side_effects=True, vmem_limit_bytes=60 * 1024 * 1024
        ),
    )(
        observations, owner_device.reshape(1, obs_rows), local_cell.reshape(1, obs_rows),
        valid_counts, weight_in, bias_in.reshape(1, hidden_size), weight_out, kernel_taps, cotangent,
    )
    grid_out, grad_in, grad_bias, grad_out, grad_kernel = out
    return (grid_out, grad_in, grad_bias.reshape(hidden_size), grad_out, grad_kernel)


def solution(mesh):
    return jax.shard_map(
        local,
        mesh=mesh,
        in_specs=(
            P(("lat", "lon"), None),
            P(("lat", "lon"), None),
            P(("lat", "lon")),
            P(("lat", "lon")),
            P(),
            P(),
            P(),
            P(),
            P(("lat", "lon"), None, None),
        ),
        out_specs=(P(("lat", "lon"), None, None), P(), P(), P(), P()),
        check_vma=False,
    )
```

```python
import functools
import math

import jax
import jax.numpy as jnp
from jax import lax
from jax.experimental import pallas as pl
from jax.experimental.pallas import tpu as pltpu
from jax.sharding import PartitionSpec as P

MESH = pl.DeviceIdType.MESH
F32 = jnp.float32
BF16 = jnp.bfloat16
OFFSETS = [(a, b) for a in (-1, 0, 1) for b in (-1, 0, 1)]
CURVE = math.sqrt(2.0 / math.pi)
META = 16
GROUP = 4


def round_up(value, step):
    return -(-value // step) * step


def iota(shape, dim):
    return lax.broadcasted_iota(jnp.int32, shape, dim)


def dot(left, right, contract=((1,), (0,))):
    return lax.dot_general(left, right, (contract, ((), ())), preferred_element_type=F32)


def kernel(
    n_lat, n_lon, slots, piece, scale,
    obs, owner, cell, count, w_in, b_in, w_out, taps, cot,
    grid_o, gin_o, gb_o, gout_o, gk_o,
    meta, slot_row, sbuf, rbuf, cot_top, cot_bot, adj_s, adj_r, adj_f, adj_b,
    dep, dep_b, dep_r, hal_top, hal_bot, strip, total, rounded, parts, gathered, gk_s, gk_lon, gk_lat,
    row_send, row_recv, cot_send, cot_recv, adj_send, adj_recv, dep_send, dep_recv,
    hal_send, hal_recv, sum_send, sum_recv, all_send, all_recv, gk_send, gk_recv,
):
    n = n_lat * n_lon
    lat, lon = lax.axis_index("lat"), lax.axis_index("lon")
    me = lat * n_lon + lon
    obs_rows, feat = obs.shape
    own_rows, cols, channels = cot.shape
    tile_rows = own_rows * n_lon
    tile_cols = cols // n_lon
    cells = tile_rows * tile_cols
    hidden_size = w_in.shape[1]
    groups = n // GROUP
    used = -(-(hidden_size + feat + 16) // piece)

    def place(target):
        return (target // n_lon, lax.rem(target, n_lon))

    def partner(turn):
        return (lax.rem(lat + lax.rem(turn, n_lat), n_lat), lax.rem(lon + turn // n_lat, n_lon))

    def number(turn):
        to_lat, to_lon = partner(turn)
        return to_lat * n_lon + to_lon

    def remote(src, dst, send, recv, device):
        return pltpu.make_async_remote_copy(
            src_ref=src, dst_ref=dst, send_sem=send, recv_sem=recv,
            device_id=device, device_id_type=MESH,
        )

    def drain(ref, sem):
        pltpu.make_async_copy(ref, ref, sem).wait()

    barrier = pltpu.get_barrier_semaphore()

    def greet(off, carry):
        pl.semaphore_signal(
            barrier, inc=1, device_id=place(lax.rem(me + off, n)), device_id_type=MESH
        )
        return carry

    lax.fori_loop(1, n, greet, 0)

    @pl.when(me == 0)
    def _():
        cot_top[...] = jnp.zeros_like(cot_top)

    @pl.when(me == n - 1)
    def _():
        cot_bot[...] = jnp.zeros_like(cot_bot)

    has_top = jnp.logical_and(lon == 0, lat > 0)
    has_bot = jnp.logical_and(lon == n_lon - 1, lat < n_lat - 1)

    @pl.when(jnp.logical_not(has_top))
    def _():
        hal_top[...] = jnp.zeros_like(hal_top)

    @pl.when(jnp.logical_not(has_bot))
    def _():
        hal_bot[...] = jnp.zeros_like(hal_bot)

    dep[...] = jnp.zeros_like(dep)
    total[...] = jnp.zeros_like(total)
    dep_b[0] = jnp.zeros((tile_cols, channels), BF16)
    dep_b[tile_rows + 1] = jnp.zeros((tile_cols, channels), BF16)

    own_row = owner[...]
    match = (own_row == iota((n, obs_rows), 0)).astype(F32)
    block = 256 if obs_rows % 256 == 0 else 128
    upper = (iota((block, block), 0) < iota((block, block), 1)).astype(F32).astype(BF16)
    carry = jnp.zeros((n, 1), F32)
    ranks = []
    for start in range(0, obs_rows, block):
        part = match[:, start:start + block]
        before = dot(part.astype(BF16), upper) + carry
        ranks.append(jnp.sum(before * part, axis=0, keepdims=True))
        carry = carry + jnp.sum(part, axis=1, keepdims=True)
    rank = jnp.concatenate(ranks, axis=1).astype(jnp.int32)
    slot_row[...] = own_row * slots + rank
    lane = iota((1, obs_rows), 1)
    code = jnp.where(lane < count[0], cell[...] + 1, 0)
    high = (code // 128).astype(F32)
    low = lax.rem(code, 128).astype(F32)
    coded = jnp.concatenate([match * high, match * low], axis=0).astype(BF16)
    by_rank = (rank == iota((128, obs_rows), 0)).astype(F32).astype(BF16)
    meta[...] = dot(coded, by_rank, ((1,), (1,)))

    pl.semaphore_wait(barrier, n - 1)

    up_copy = remote(cot.at[own_rows - 1], cot_top, cot_send.at[0], cot_recv.at[0], place(lax.rem(me + 1, n)))
    down_copy = remote(cot.at[0], cot_bot, cot_send.at[1], cot_recv.at[1], place(lax.rem(me + n - 1, n)))

    @pl.when(me < n - 1)
    def _():
        up_copy.start()

    @pl.when(me > 0)
    def _():
        down_copy.start()

    def row_copy(off, g):
        return remote(
            sbuf.at[off], rbuf.at[off], row_send, row_recv.at[g], partner(off)
        )

    def send_group(g, carry, first=False):
        ids = slot_row[...]
        picks = []
        for q in range(GROUP):
            target = number(g * GROUP + q)
            pick = (ids - target * slots) == iota((slots, obs_rows), 0)
            picks.append(pick.astype(F32).astype(BF16))
        rows = dot(jnp.concatenate(picks, axis=0), obs[...]).astype(BF16)
        line = iota((META, 128), 0)
        for q in range(GROUP):
            off = g * GROUP + q
            target = number(off)
            sbuf[off, :slots, :] = rows[q * slots:(q + 1) * slots]
            tail = jnp.where(
                line == 0, meta[pl.ds(target, 1), :],
                jnp.where(line == 1, meta[pl.ds(n + target, 1), :], 0.0),
            )
            sbuf[off, slots:slots + META, :] = tail.astype(BF16)
        for q in range(GROUP):
            if first and q == 0:
                pltpu.make_async_copy(sbuf.at[0], rbuf.at[0], row_recv.at[0]).start()
            else:
                row_copy(g * GROUP + q, g).start()
        return carry

    send_group(0, 0, True)

    @pl.when(me > 0)
    def _():
        up_copy.wait_recv()

    @pl.when(me < n - 1)
    def _():
        down_copy.wait_recv()

    tap = taps[...]

    def shifts(row):
        return {0: row, 1: pltpu.roll(row, 1, 0), -1: pltpu.roll(row, cols - 1, 0)}

    cot_rows = [cot_top[...]] + [cot[r] for r in range(own_rows)] + [cot_bot[...]]
    sums = [jnp.zeros((cols, channels), F32) for _ in range(own_rows)]
    for at, row in enumerate(cot_rows):
        moved = shifts(row.astype(F32))
        for y in range(own_rows):
            a = y - (at - 1)
            if abs(a) <= 1:
                for b in (-1, 0, 1):
                    k = 3 * (a + 1) + b + 1
                    sums[y] = sums[y] + tap[k:k + 1] * moved[b]
    for y in range(own_rows):
        value = scale * sums[y]
        for j in range(n_lon):
            adj_s[j, y] = value[j * tile_cols:(j + 1) * tile_cols].astype(BF16)

    def adj_copy(step):
        other = lax.rem(lon + step, n_lon)
        return remote(
            adj_s.at[other], adj_r.at[lon], adj_send, adj_recv, (lat, other)
        )

    for step in range(1, n_lon):
        adj_copy(step).start()
    adj_r[lon] = adj_s[lon]

    lax.fori_loop(1, groups, send_group, 0)

    drain(adj_r.at[pl.ds(0, n_lon - 1)], adj_recv)
    for k in range(n_lon):
        for y in range(own_rows):
            m = k * own_rows + y
            adj_f[m * tile_cols:(m + 1) * tile_cols, :] = adj_r[k, y].astype(F32)
    adj_b[...] = adj_f[...].astype(BF16)

    bias_at = hidden_size + feat

    def take_group(g, carry):
        held = rbuf.at[pl.ds(g * GROUP, GROUP)]
        drain(held, row_recv.at[g])
        rows = jnp.concatenate([rbuf[g * GROUP + q, :slots, :] for q in range(GROUP)], axis=0)
        same = iota((slots, 128), 0) == iota((slots, 128), 1)
        spread = []
        for q in range(GROUP):
            tail = rbuf[g * GROUP + q, slots:slots + META, :].astype(F32)
            spread.append(jnp.concatenate(
                [jnp.where(same, tail[0:1], 0.0), jnp.where(same, tail[1:2], 0.0)], axis=1
            ).astype(BF16))
        weigh = jnp.where(iota((256, 128), 0) < 128, 128.0, 1.0).astype(BF16)
        codes = dot(jnp.concatenate(spread, axis=0), weigh).astype(jnp.int32)
        lanes = iota(codes.shape, 1) + 1
        pick = jnp.concatenate(
            [(codes == lanes + at).astype(F32).astype(BF16) for at in range(0, cells, 128)], axis=1
        )
        x = dot(rows, w_in[...]) + b_in[...]
        square = x * x
        t = jnp.tanh(CURVE * (x + 0.044715 * (square * x)))
        half = 0.5 * (1.0 + t)
        hidden = (x * half).astype(BF16)
        slope = half + 0.5 * x * (1.0 - t * t) * (CURVE * (1.0 + 3.0 * 0.044715 * square))
        encoded = dot(hidden, w_out[...]).astype(BF16)
        dep[...] += dot(pick, encoded, ((0,), (0,)))
        upstream = dot(pick, adj_b[...]).astype(BF16)
        back = dot(upstream, w_out[...], ((1,), (1,)))
        pre = (back * slope).astype(BF16)
        total[0:hidden_size, :] += dot(hidden, upstream, ((0,), (0,)))
        total[hidden_size:bias_at, :] += dot(rows, pre, ((0,), (0,)))
        total[bias_at:bias_at + 1, :] += jnp.sum(pre.astype(F32), axis=0, keepdims=True)
        return carry

    lax.fori_loop(0, groups, take_group, 0)

    for m in range(tile_rows):
        dep_b[m + 1] = dep[m * tile_cols:(m + 1) * tile_cols, :].astype(BF16)

    def dep_copy(step):
        other = lax.rem(lon + step, n_lon)
        return remote(
            dep_b.at[pl.ds(other * own_rows, own_rows + 2)], dep_r.at[lon],
            dep_send, dep_recv, (lat, other),
        )

    low_copy = remote(
        dep_b.at[tile_rows], hal_top.at[lon], hal_send.at[0], hal_recv.at[0],
        (lax.rem(lat + 1, n_lat), 0),
    )
    high_copy = remote(
        dep_b.at[1], hal_bot.at[lon], hal_send.at[1], hal_recv.at[1],
        (lax.rem(lat + n_lat - 1, n_lat), n_lon - 1),
    )

    @pl.when(lat < n_lat - 1)
    def _():
        low_copy.start()

    @pl.when(lat > 0)
    def _():
        high_copy.start()

    for step in range(1, n_lon):
        dep_copy(step).start()
    dep_r[lon] = dep_b[pl.ds(lon * own_rows, own_rows + 2)]

    def span(at):
        return pl.ds(pl.multiple_of(at * piece, 16), piece)

    def sum_start(off, carry):
        target = number(off)

        @pl.when(target < used)
        def _():
            remote(
                rounded.at[span(target)], parts.at[off - 1], sum_send, sum_recv, partner(off)
            ).start()

        return carry

    rounded[...] = total[...].astype(BF16)
    lax.fori_loop(1, n, sum_start, 0)

    drain(dep_r.at[pl.ds(0, n_lon - 1)], dep_recv)

    @pl.when(has_top)
    def _():
        drain(hal_top, hal_recv.at[0])

    @pl.when(has_bot)
    def _():
        drain(hal_bot, hal_recv.at[1])

    for j in range(n_lon):
        for r in range(own_rows + 2):
            value = dep_r[j, r].astype(F32)
            if r == 0:
                value = value + hal_top[j].astype(F32)
            if r == own_rows + 1:
                value = value + hal_bot[j].astype(F32)
            strip[r, j * tile_cols:(j + 1) * tile_cols, :] = value

    fields = [jnp.zeros((cols, channels), F32) for _ in range(own_rows)]
    kernel_rows = [jnp.zeros((1, channels), F32) for _ in OFFSETS]
    for at in range(own_rows + 2):
        moved = shifts(strip[at])
        for y in range(own_rows):
            a = at - 1 - y
            if abs(a) <= 1:
                for b in (-1, 0, 1):
                    k = 3 * (a + 1) + b + 1
                    fields[y] = fields[y] + tap[k:k + 1] * moved[-b]
                    kernel_rows[k] = kernel_rows[k] + jnp.sum(
                        cot[y].astype(F32) * moved[-b], axis=0, keepdims=True
                    )
    for y in range(own_rows):
        grid_o[y] = fields[y].astype(BF16)
    spare = gk_s.shape[1] - len(OFFSETS)
    grad_taps = scale * jnp.concatenate(kernel_rows + [jnp.zeros((spare, channels), F32)], axis=0)
    gk_s[0] = grad_taps.astype(BF16)
    for step in range(1, n_lon):
        remote(
            gk_s.at[0], gk_lon.at[lon], gk_send.at[0], gk_recv.at[0],
            (lat, lax.rem(lon + step, n_lon)),
        ).start()

    @pl.when(me < used)
    def _():
        drain(parts, sum_recv)

        def add_part(at, value):
            return value + parts[at].astype(F32)

        gathered[span(me), :] = lax.fori_loop(
            0, n - 1, add_part, total[span(me), :]
        ).astype(BF16)

        def all_start(off, carry):
            remote(
                gathered.at[span(me)], gathered.at[span(me)], all_send, all_recv, partner(off)
            ).start()
            return carry

        lax.fori_loop(1, n, all_start, 0)

    gk_lon[lon] = gk_s[0]
    drain(gk_lon.at[pl.ds(0, n_lon - 1)], gk_recv.at[0])
    grad_taps = gk_lon[0].astype(F32)
    for at in range(1, n_lon):
        grad_taps = grad_taps + gk_lon[at].astype(F32)
    gk_s[1] = grad_taps.astype(BF16)
    for step in range(1, n_lat):
        remote(
            gk_s.at[1], gk_lat.at[lat], gk_send.at[1], gk_recv.at[1],
            (lax.rem(lat + step, n_lat), lon),
        ).start()
    gk_lat[lat] = gk_s[1]
    drain(gk_lat.at[pl.ds(0, n_lat - 1)], gk_recv.at[1])
    grad_taps = gk_lat[0].astype(F32)
    for at in range(1, n_lat):
        grad_taps = grad_taps + gk_lat[at].astype(F32)
    gk_o[...] = grad_taps[0:len(OFFSETS)]

    @pl.when(me < used)
    def _():
        drain(gathered.at[pl.ds(0, (used - 1) * piece)], all_recv)

    @pl.when(me >= used)
    def _():
        drain(gathered.at[pl.ds(0, used * piece)], all_recv)

    gout_o[...] = gathered[0:hidden_size, :].astype(F32)
    gin_o[...] = gathered[hidden_size:bias_at, :].astype(F32)
    gb_o[...] = gathered[bias_at:bias_at + 16, :].astype(F32)[0:1]

    drain(sbuf.at[pl.ds(0, n - 1)], row_send)
    drain(adj_s.at[pl.ds(0, n_lon - 1)], adj_send)
    drain(dep_r.at[pl.ds(0, n_lon - 1)], dep_send)
    drain(gk_lon.at[pl.ds(0, n_lon - 1)], gk_send.at[0])
    drain(gk_lat.at[pl.ds(0, n_lat - 1)], gk_send.at[1])

    @pl.when(me < used)
    def _():
        drain(gathered.at[pl.ds(0, (used - 1) * piece)], sum_send)
        drain(gathered.at[pl.ds(0, (n - 1) * piece)], all_send)

    @pl.when(me >= used)
    def _():
        drain(gathered.at[pl.ds(0, used * piece)], sum_send)

    @pl.when(me < n - 1)
    def _():
        up_copy.wait_send()

    @pl.when(me > 0)
    def _():
        down_copy.wait_send()

    @pl.when(lat < n_lat - 1)
    def _():
        low_copy.wait_send()

    @pl.when(lat > 0)
    def _():
        high_copy.wait_send()


def local(
    observations, owner_device, local_cell, valid_counts,
    weight_in, bias_in, weight_out, kernel_taps, cotangent,
):
    n_lat, n_lon = lax.axis_size("lat"), lax.axis_size("lon")
    n = n_lat * n_lon
    obs_rows, feat = observations.shape
    hidden_size, channels = weight_out.shape
    own_rows, cols, _ = cotangent.shape
    tile_rows, tile_cols = own_rows * n_lon, cols // n_lon
    cells = tile_rows * tile_cols
    slots = round_up(2 * obs_rows // n, 16)
    piece = round_up(-(-(hidden_size + feat + 16) // n), 16)
    taps = kernel_taps.shape[0]
    kernel_pad = round_up(taps, 16)
    scale = 1.0 / math.sqrt(obs_rows * n)
    vmem = pl.BlockSpec(memory_space=pltpu.VMEM)
    dma = pltpu.SemaphoreType.DMA
    out = pl.pallas_call(
        functools.partial(kernel, n_lat, n_lon, slots, piece, scale),
        out_shape=(
            jax.ShapeDtypeStruct(cotangent.shape, BF16),
            jax.ShapeDtypeStruct((feat, hidden_size), F32),
            jax.ShapeDtypeStruct((1, hidden_size), F32),
            jax.ShapeDtypeStruct((hidden_size, channels), F32),
            jax.ShapeDtypeStruct((taps, channels), F32),
        ),
        in_specs=[vmem, vmem, vmem, pl.BlockSpec(memory_space=pltpu.SMEM)] + [vmem] * 5,
        out_specs=(vmem,) * 5,
        scratch_shapes=[
            pltpu.VMEM((2 * n, 128), F32),
            pltpu.VMEM((1, obs_rows), jnp.int32),
            pltpu.VMEM((n, slots + META, feat), BF16),
            pltpu.VMEM((n, slots + META, feat), BF16),
            pltpu.VMEM((cols, channels), BF16),
            pltpu.VMEM((cols, channels), BF16),
            pltpu.VMEM((n_lon, own_rows, tile_cols, channels), BF16),
            pltpu.VMEM((n_lon, own_rows, tile_cols, channels), BF16),
            pltpu.VMEM((cells, channels), F32),
            pltpu.VMEM((cells, channels), BF16),
            pltpu.VMEM((cells, channels), F32),
            pltpu.VMEM((tile_rows + 2, tile_cols, channels), BF16),
            pltpu.VMEM((n_lon, own_rows + 2, tile_cols, channels), BF16),
            pltpu.VMEM((n_lon, tile_cols, channels), BF16),
            pltpu.VMEM((n_lon, tile_cols, channels), BF16),
            pltpu.VMEM((own_rows + 2, cols, channels), F32),
            pltpu.VMEM((n * piece, channels), F32),
            pltpu.VMEM((n * piece, channels), BF16),
            pltpu.VMEM((n - 1, piece, channels), BF16),
            pltpu.VMEM((n * piece, channels), BF16),
            pltpu.VMEM((2, kernel_pad, channels), BF16),
            pltpu.VMEM((n_lon, kernel_pad, channels), BF16),
            pltpu.VMEM((n_lat, kernel_pad, channels), BF16),
            dma, dma((n // GROUP,)), dma((2,)), dma((2,)), dma, dma, dma, dma,
            dma((2,)), dma((2,)), dma, dma, dma, dma, dma((2,)), dma((2,)),
        ],
        compiler_params=pltpu.CompilerParams(
            collective_id=0, has_side_effects=True, vmem_limit_bytes=60 * 1024 * 1024
        ),
    )(
        observations, owner_device.reshape(1, obs_rows), local_cell.reshape(1, obs_rows),
        valid_counts, weight_in, bias_in.reshape(1, hidden_size), weight_out, kernel_taps, cotangent,
    )
    grid_out, grad_in, grad_bias, grad_out, grad_kernel = out
    return (grid_out, grad_in, grad_bias.reshape(hidden_size), grad_out, grad_kernel)


def solution(mesh):
    return jax.shard_map(
        local,
        mesh=mesh,
        in_specs=(
            P(("lat", "lon"), None),
            P(("lat", "lon"), None),
            P(("lat", "lon")),
            P(("lat", "lon")),
            P(),
            P(),
            P(),
            P(),
            P(("lat", "lon"), None, None),
        ),
        out_specs=(P(("lat", "lon"), None, None), P(), P(), P(), P()),
        check_vma=False,
    )
```

```python
import functools
import math

import jax
import jax.numpy as jnp
from jax import lax
from jax.experimental import pallas as pl
from jax.experimental.pallas import tpu as pltpu
from jax.sharding import PartitionSpec as P

MESH = pl.DeviceIdType.MESH
F32 = jnp.float32
BF16 = jnp.bfloat16
OFFSETS = [(a, b) for a in (-1, 0, 1) for b in (-1, 0, 1)]
CURVE = math.sqrt(2.0 / math.pi)
META = 16
GROUP = 4


def round_up(value, step):
    return -(-value // step) * step


def iota(shape, dim):
    return lax.broadcasted_iota(jnp.int32, shape, dim)


def dot(left, right, contract=((1,), (0,))):
    return lax.dot_general(left, right, (contract, ((), ())), preferred_element_type=F32)


def kernel(
    n_lat, n_lon, slots, piece, scale,
    obs, owner, cell, count, w_in, b_in, w_out, taps, cot,
    grid_o, gin_o, gb_o, gout_o, gk_o,
    meta, slot_row, sbuf, rbuf, cot_top, cot_bot, adj_s, adj_r, adj_f, adj_b,
    dep, dep_b, dep_r, hal_top, hal_bot, strip, total, rounded, parts, gathered, gk_s, gk_lon, gk_lat,
    row_send, row_recv, cot_send, cot_recv, adj_send, adj_recv, dep_send, dep_recv,
    hal_send, hal_recv, sum_send, sum_recv, all_send, all_recv, gk_send, gk_recv,
):
    n = n_lat * n_lon
    lat, lon = lax.axis_index("lat"), lax.axis_index("lon")
    me = lat * n_lon + lon
    obs_rows, feat = obs.shape
    own_rows, cols, channels = cot.shape
    tile_rows = own_rows * n_lon
    tile_cols = cols // n_lon
    cells = tile_rows * tile_cols
    hidden_size = w_in.shape[1]
    groups = n // GROUP
    used = -(-(hidden_size + feat + 16) // piece)

    def place(target):
        return (target // n_lon, lax.rem(target, n_lon))

    def partner(turn):
        return (lax.rem(lat + lax.rem(turn, n_lat), n_lat), lax.rem(lon + turn // n_lat, n_lon))

    def number(turn):
        to_lat, to_lon = partner(turn)
        return to_lat * n_lon + to_lon

    def remote(src, dst, send, recv, device):
        return pltpu.make_async_remote_copy(
            src_ref=src, dst_ref=dst, send_sem=send, recv_sem=recv,
            device_id=device, device_id_type=MESH,
        )

    def drain(ref, sem):
        pltpu.make_async_copy(ref, ref, sem).wait()

    barrier = pltpu.get_barrier_semaphore()

    def greet(off, carry):
        pl.semaphore_signal(
            barrier, inc=1, device_id=place(lax.rem(me + off, n)), device_id_type=MESH
        )
        return carry

    lax.fori_loop(1, n, greet, 0)

    @pl.when(me == 0)
    def _():
        cot_top[...] = jnp.zeros_like(cot_top)

    @pl.when(me == n - 1)
    def _():
        cot_bot[...] = jnp.zeros_like(cot_bot)

    has_top = jnp.logical_and(lon == 0, lat > 0)
    has_bot = jnp.logical_and(lon == n_lon - 1, lat < n_lat - 1)

    @pl.when(jnp.logical_not(has_top))
    def _():
        hal_top[...] = jnp.zeros_like(hal_top)

    @pl.when(jnp.logical_not(has_bot))
    def _():
        hal_bot[...] = jnp.zeros_like(hal_bot)

    dep[...] = jnp.zeros_like(dep)
    total[...] = jnp.zeros_like(total)
    dep_b[0] = jnp.zeros((tile_cols, channels), BF16)
    dep_b[tile_rows + 1] = jnp.zeros((tile_cols, channels), BF16)

    own_row = owner[...]
    match = (own_row == iota((n, obs_rows), 0)).astype(F32)
    block = 256 if obs_rows % 256 == 0 else 128
    upper = (iota((block, block), 0) < iota((block, block), 1)).astype(F32).astype(BF16)
    carry = jnp.zeros((n, 1), F32)
    ranks = []
    for start in range(0, obs_rows, block):
        part = match[:, start:start + block]
        before = dot(part.astype(BF16), upper) + carry
        ranks.append(jnp.sum(before * part, axis=0, keepdims=True))
        carry = carry + jnp.sum(part, axis=1, keepdims=True)
    rank = jnp.concatenate(ranks, axis=1).astype(jnp.int32)
    slot_row[...] = own_row * slots + rank
    lane = iota((1, obs_rows), 1)
    code = jnp.where(lane < count[0], cell[...] + 1, 0)
    high = (code // 128).astype(F32)
    low = lax.rem(code, 128).astype(F32)
    coded = jnp.concatenate([match * high, match * low], axis=0).astype(BF16)
    by_rank = (rank == iota((128, obs_rows), 0)).astype(F32).astype(BF16)
    meta[...] = dot(coded, by_rank, ((1,), (1,)))

    pl.semaphore_wait(barrier, n - 1)

    up_copy = remote(cot.at[own_rows - 1], cot_top, cot_send.at[0], cot_recv.at[0], place(lax.rem(me + 1, n)))
    down_copy = remote(cot.at[0], cot_bot, cot_send.at[1], cot_recv.at[1], place(lax.rem(me + n - 1, n)))

    @pl.when(me < n - 1)
    def _():
        up_copy.start()

    @pl.when(me > 0)
    def _():
        down_copy.start()

    def row_copy(off, g):
        return remote(
            sbuf.at[off], rbuf.at[off], row_send, row_recv.at[g], partner(off)
        )

    def send_group(g, carry, first=False):
        ids = slot_row[...]
        picks = []
        for q in range(GROUP):
            target = number(g * GROUP + q)
            pick = (ids - target * slots) == iota((slots, obs_rows), 0)
            picks.append(pick.astype(F32).astype(BF16))
        rows = dot(jnp.concatenate(picks, axis=0), obs[...]).astype(BF16)
        line = iota((META, 128), 0)
        for q in range(GROUP):
            off = g * GROUP + q
            target = number(off)
            sbuf[off, :slots, :] = rows[q * slots:(q + 1) * slots]
            tail = jnp.where(
                line == 0, meta[pl.ds(target, 1), :],
                jnp.where(line == 1, meta[pl.ds(n + target, 1), :], 0.0),
            )
            sbuf[off, slots:slots + META, :] = tail.astype(BF16)
        for q in range(GROUP):
            if first and q == 0:
                pltpu.make_async_copy(sbuf.at[0], rbuf.at[0], row_recv.at[0]).start()
            else:
                row_copy(g * GROUP + q, g).start()
        return carry

    send_group(0, 0, True)
    lax.fori_loop(1, groups, send_group, 0)

    @pl.when(me > 0)
    def _():
        up_copy.wait_recv()

    @pl.when(me < n - 1)
    def _():
        down_copy.wait_recv()

    tap = taps[...]

    def shifts(row):
        return {0: row, 1: pltpu.roll(row, 1, 0), -1: pltpu.roll(row, cols - 1, 0)}

    cot_rows = [cot_top[...]] + [cot[r] for r in range(own_rows)] + [cot_bot[...]]
    sums = [jnp.zeros((cols, channels), F32) for _ in range(own_rows)]
    for at, row in enumerate(cot_rows):
        moved = shifts(row.astype(F32))
        for y in range(own_rows):
            a = y - (at - 1)
            if abs(a) <= 1:
                for b in (-1, 0, 1):
                    k = 3 * (a + 1) + b + 1
                    sums[y] = sums[y] + tap[k:k + 1] * moved[b]
    for y in range(own_rows):
        value = scale * sums[y]
        for j in range(n_lon):
            adj_s[j, y] = value[j * tile_cols:(j + 1) * tile_cols].astype(BF16)

    def adj_copy(step):
        other = lax.rem(lon + step, n_lon)
        return remote(
            adj_s.at[other], adj_r.at[lon], adj_send, adj_recv, (lat, other)
        )

    for step in range(1, n_lon):
        adj_copy(step).start()
    adj_r[lon] = adj_s[lon]

    drain(adj_r.at[pl.ds(0, n_lon - 1)], adj_recv)
    for k in range(n_lon):
        for y in range(own_rows):
            m = k * own_rows + y
            adj_f[m * tile_cols:(m + 1) * tile_cols, :] = adj_r[k, y].astype(F32)
    adj_b[...] = adj_f[...].astype(BF16)

    bias_at = hidden_size + feat

    def take_group(g, carry):
        held = rbuf.at[pl.ds(g * GROUP, GROUP)]
        drain(held, row_recv.at[g])
        rows = jnp.concatenate([rbuf[g * GROUP + q, :slots, :] for q in range(GROUP)], axis=0)
        same = iota((slots, 128), 0) == iota((slots, 128), 1)
        spread = []
        for q in range(GROUP):
            tail = rbuf[g * GROUP + q, slots:slots + META, :].astype(F32)
            spread.append(jnp.concatenate(
                [jnp.where(same, tail[0:1], 0.0), jnp.where(same, tail[1:2], 0.0)], axis=1
            ).astype(BF16))
        weigh = jnp.where(iota((256, 128), 0) < 128, 128.0, 1.0).astype(BF16)
        codes = dot(jnp.concatenate(spread, axis=0), weigh).astype(jnp.int32)
        lanes = iota(codes.shape, 1) + 1
        pick = jnp.concatenate(
            [(codes == lanes + at).astype(F32).astype(BF16) for at in range(0, cells, 128)], axis=1
        )
        x = dot(rows, w_in[...]) + b_in[...]
        square = x * x
        t = jnp.tanh(CURVE * (x + 0.044715 * (square * x)))
        half = 0.5 * (1.0 + t)
        hidden = (x * half).astype(BF16)
        slope = half + 0.5 * x * (1.0 - t * t) * (CURVE * (1.0 + 3.0 * 0.044715 * square))
        encoded = dot(hidden, w_out[...]).astype(BF16)
        dep[...] += dot(pick, encoded, ((0,), (0,)))
        upstream = dot(pick, adj_b[...]).astype(BF16)
        back = dot(upstream, w_out[...], ((1,), (1,)))
        pre = (back * slope).astype(BF16)
        total[0:hidden_size, :] += dot(hidden, upstream, ((0,), (0,)))
        total[hidden_size:bias_at, :] += dot(rows, pre, ((0,), (0,)))
        total[bias_at:bias_at + 1, :] += jnp.sum(pre.astype(F32), axis=0, keepdims=True)
        return carry

    lax.fori_loop(0, groups, take_group, 0)

    for m in range(tile_rows):
        dep_b[m + 1] = dep[m * tile_cols:(m + 1) * tile_cols, :].astype(BF16)

    def dep_copy(step):
        other = lax.rem(lon + step, n_lon)
        return remote(
            dep_b.at[pl.ds(other * own_rows, own_rows + 2)], dep_r.at[lon],
            dep_send, dep_recv, (lat, other),
        )

    low_copy = remote(
        dep_b.at[tile_rows], hal_top.at[lon], hal_send.at[0], hal_recv.at[0],
        (lax.rem(lat + 1, n_lat), 0),
    )
    high_copy = remote(
        dep_b.at[1], hal_bot.at[lon], hal_send.at[1], hal_recv.at[1],
        (lax.rem(lat + n_lat - 1, n_lat), n_lon - 1),
    )

    @pl.when(lat < n_lat - 1)
    def _():
        low_copy.start()

    @pl.when(lat > 0)
    def _():
        high_copy.start()

    for step in range(1, n_lon):
        dep_copy(step).start()
    dep_r[lon] = dep_b[pl.ds(lon * own_rows, own_rows + 2)]

    def span(at):
        return pl.ds(pl.multiple_of(at * piece, 16), piece)

    def sum_start(off, carry):
        target = number(off)

        @pl.when(target < used)
        def _():
            remote(
                rounded.at[span(target)], parts.at[off - 1], sum_send, sum_recv, partner(off)
            ).start()

        return carry

    rounded[...] = total[...].astype(BF16)
    lax.fori_loop(1, n, sum_start, 0)

    drain(dep_r.at[pl.ds(0, n_lon - 1)], dep_recv)

    @pl.when(has_top)
    def _():
        drain(hal_top, hal_recv.at[0])

    @pl.when(has_bot)
    def _():
        drain(hal_bot, hal_recv.at[1])

    for j in range(n_lon):
        for r in range(own_rows + 2):
            value = dep_r[j, r].astype(F32)
            if r == 0:
                value = value + hal_top[j].astype(F32)
            if r == own_rows + 1:
                value = value + hal_bot[j].astype(F32)
            strip[r, j * tile_cols:(j + 1) * tile_cols, :] = value

    fields = [jnp.zeros((cols, channels), F32) for _ in range(own_rows)]
    kernel_rows = [jnp.zeros((1, channels), F32) for _ in OFFSETS]
    for at in range(own_rows + 2):
        moved = shifts(strip[at])
        for y in range(own_rows):
            a = at - 1 - y
            if abs(a) <= 1:
                for b in (-1, 0, 1):
                    k = 3 * (a + 1) + b + 1
                    fields[y] = fields[y] + tap[k:k + 1] * moved[-b]
                    kernel_rows[k] = kernel_rows[k] + jnp.sum(
                        cot[y].astype(F32) * moved[-b], axis=0, keepdims=True
                    )
    for y in range(own_rows):
        grid_o[y] = fields[y].astype(BF16)
    spare = gk_s.shape[1] - len(OFFSETS)
    grad_taps = scale * jnp.concatenate(kernel_rows + [jnp.zeros((spare, channels), F32)], axis=0)
    gk_s[0] = grad_taps.astype(BF16)
    for step in range(1, n_lon):
        remote(
            gk_s.at[0], gk_lon.at[lon], gk_send.at[0], gk_recv.at[0],
            (lat, lax.rem(lon + step, n_lon)),
        ).start()

    @pl.when(me < used)
    def _():
        drain(parts, sum_recv)

        def add_part(at, value):
            return value + parts[at].astype(F32)

        gathered[span(me), :] = lax.fori_loop(
            0, n - 1, add_part, total[span(me), :]
        ).astype(BF16)

        def all_start(off, carry):
            remote(
                gathered.at[span(me)], gathered.at[span(me)], all_send, all_recv, partner(off)
            ).start()
            return carry

        lax.fori_loop(1, n, all_start, 0)

    gk_lon[lon] = gk_s[0]
    drain(gk_lon.at[pl.ds(0, n_lon - 1)], gk_recv.at[0])
    grad_taps = gk_lon[0].astype(F32)
    for at in range(1, n_lon):
        grad_taps = grad_taps + gk_lon[at].astype(F32)
    gk_s[1] = grad_taps.astype(BF16)
    for step in range(1, n_lat):
        remote(
            gk_s.at[1], gk_lat.at[lat], gk_send.at[1], gk_recv.at[1],
            (lax.rem(lat + step, n_lat), lon),
        ).start()
    gk_lat[lat] = gk_s[1]
    drain(gk_lat.at[pl.ds(0, n_lat - 1)], gk_recv.at[1])
    grad_taps = gk_lat[0].astype(F32)
    for at in range(1, n_lat):
        grad_taps = grad_taps + gk_lat[at].astype(F32)
    gk_o[...] = grad_taps[0:len(OFFSETS)]

    @pl.when(me < used)
    def _():
        drain(gathered.at[pl.ds(0, (used - 1) * piece)], all_recv)

    @pl.when(me >= used)
    def _():
        drain(gathered.at[pl.ds(0, used * piece)], all_recv)

    gout_o[...] = gathered[0:hidden_size, :].astype(F32)
    gin_o[...] = gathered[hidden_size:bias_at, :].astype(F32)
    gb_o[...] = gathered[bias_at:bias_at + 16, :].astype(F32)[0:1]

    drain(sbuf.at[pl.ds(0, n - 1)], row_send)
    drain(adj_s.at[pl.ds(0, n_lon - 1)], adj_send)
    drain(dep_r.at[pl.ds(0, n_lon - 1)], dep_send)
    drain(gk_lon.at[pl.ds(0, n_lon - 1)], gk_send.at[0])
    drain(gk_lat.at[pl.ds(0, n_lat - 1)], gk_send.at[1])

    @pl.when(me < used)
    def _():
        drain(gathered.at[pl.ds(0, (used - 1) * piece)], sum_send)
        drain(gathered.at[pl.ds(0, (n - 1) * piece)], all_send)

    @pl.when(me >= used)
    def _():
        drain(gathered.at[pl.ds(0, used * piece)], sum_send)

    @pl.when(me < n - 1)
    def _():
        up_copy.wait_send()

    @pl.when(me > 0)
    def _():
        down_copy.wait_send()

    @pl.when(lat < n_lat - 1)
    def _():
        low_copy.wait_send()

    @pl.when(lat > 0)
    def _():
        high_copy.wait_send()


def local(
    observations, owner_device, local_cell, valid_counts,
    weight_in, bias_in, weight_out, kernel_taps, cotangent,
):
    n_lat, n_lon = lax.axis_size("lat"), lax.axis_size("lon")
    n = n_lat * n_lon
    obs_rows, feat = observations.shape
    hidden_size, channels = weight_out.shape
    own_rows, cols, _ = cotangent.shape
    tile_rows, tile_cols = own_rows * n_lon, cols // n_lon
    cells = tile_rows * tile_cols
    slots = round_up(2 * obs_rows // n, 16)
    piece = round_up(-(-(hidden_size + feat + 16) // n), 16)
    taps = kernel_taps.shape[0]
    kernel_pad = round_up(taps, 16)
    scale = 1.0 / math.sqrt(obs_rows * n)
    vmem = pl.BlockSpec(memory_space=pltpu.VMEM)
    dma = pltpu.SemaphoreType.DMA
    out = pl.pallas_call(
        functools.partial(kernel, n_lat, n_lon, slots, piece, scale),
        out_shape=(
            jax.ShapeDtypeStruct(cotangent.shape, BF16),
            jax.ShapeDtypeStruct((feat, hidden_size), F32),
            jax.ShapeDtypeStruct((1, hidden_size), F32),
            jax.ShapeDtypeStruct((hidden_size, channels), F32),
            jax.ShapeDtypeStruct((taps, channels), F32),
        ),
        in_specs=[vmem, vmem, vmem, pl.BlockSpec(memory_space=pltpu.SMEM)] + [vmem] * 5,
        out_specs=(vmem,) * 5,
        scratch_shapes=[
            pltpu.VMEM((2 * n, 128), F32),
            pltpu.VMEM((1, obs_rows), jnp.int32),
            pltpu.VMEM((n, slots + META, feat), BF16),
            pltpu.VMEM((n, slots + META, feat), BF16),
            pltpu.VMEM((cols, channels), BF16),
            pltpu.VMEM((cols, channels), BF16),
            pltpu.VMEM((n_lon, own_rows, tile_cols, channels), BF16),
            pltpu.VMEM((n_lon, own_rows, tile_cols, channels), BF16),
            pltpu.VMEM((cells, channels), F32),
            pltpu.VMEM((cells, channels), BF16),
            pltpu.VMEM((cells, channels), F32),
            pltpu.VMEM((tile_rows + 2, tile_cols, channels), BF16),
            pltpu.VMEM((n_lon, own_rows + 2, tile_cols, channels), BF16),
            pltpu.VMEM((n_lon, tile_cols, channels), BF16),
            pltpu.VMEM((n_lon, tile_cols, channels), BF16),
            pltpu.VMEM((own_rows + 2, cols, channels), F32),
            pltpu.VMEM((n * piece, channels), F32),
            pltpu.VMEM((n * piece, channels), BF16),
            pltpu.VMEM((n - 1, piece, channels), BF16),
            pltpu.VMEM((n * piece, channels), BF16),
            pltpu.VMEM((2, kernel_pad, channels), BF16),
            pltpu.VMEM((n_lon, kernel_pad, channels), BF16),
            pltpu.VMEM((n_lat, kernel_pad, channels), BF16),
            dma, dma((n // GROUP,)), dma((2,)), dma((2,)), dma, dma, dma, dma,
            dma((2,)), dma((2,)), dma, dma, dma, dma, dma((2,)), dma((2,)),
        ],
        compiler_params=pltpu.CompilerParams(
            collective_id=0, has_side_effects=True, vmem_limit_bytes=60 * 1024 * 1024
        ),
    )(
        observations, owner_device.reshape(1, obs_rows), local_cell.reshape(1, obs_rows),
        valid_counts, weight_in, bias_in.reshape(1, hidden_size), weight_out, kernel_taps, cotangent,
    )
    grid_out, grad_in, grad_bias, grad_out, grad_kernel = out
    return (grid_out, grad_in, grad_bias.reshape(hidden_size), grad_out, grad_kernel)


def solution(mesh):
    return jax.shard_map(
        local,
        mesh=mesh,
        in_specs=(
            P(("lat", "lon"), None),
            P(("lat", "lon"), None),
            P(("lat", "lon")),
            P(("lat", "lon")),
            P(),
            P(),
            P(),
            P(),
            P(("lat", "lon"), None, None),
        ),
        out_specs=(P(("lat", "lon"), None, None), P(), P(), P(), P()),
        check_vma=False,
    )
```
